32 devices in a mesh: dp: 8 (over y, x, core), expert: 4 (over z).
Axes of the slice: x: 2, y: 2, z: 4, core: 2. Of those that a mesh axis runs over, the one named last changes fastest.
Arguments:
- grad_out: bfloat16 [4, 2048, 1024], P(None, ('dp', 'expert')), may hold values from -12 to 12
- routes: int32 [4, 2048, 8], P(None, ('dp', 'expert')), may hold values from 0 to 127, all different within a row; in each aligned block of 64 rows (0 to 63, 64 to 127, ..., all dimensions but the last counted through in order) at most 8 rows name the same one
- route_probs: bfloat16 [4, 2048, 8], P(None, ('dp', 'expert')), may hold values from 0.049804688 to 0.3984375
- dispatched: bfloat16 [4, 1024, 1024], P(None, ('dp', 'expert')), may hold values from -12 to 12, as said below
- w_gate: bfloat16 [1024, 1024], P(None, 'expert'), may hold values from -0.1875 to 0.1875
- w_up: bfloat16 [1024, 1024], P(None, 'expert'), may hold values from -0.1875 to 0.1875
- w_down: bfloat16 [1024, 1024], P('expert'), may hold values from -0.25 to 0.25
Outputs:
- grad_in: bfloat16 [4, 2048, 1024], P(None, ('dp', 'expert'))
- grad_gate: float32 [1024, 1024], P('dp', 'expert')
- grad_up: float32 [1024, 1024], P('dp', 'expert')
- grad_down_t: float32 [1024, 1024], P('dp', 'expert')
The draws below stay inside these ranges and needn't reach their ends.
Inputs may be any that keep to these rules, and one draw needn't show every extreme that they name: `routes`: in each micro-batch, among the 64 rows of one device no expert is named more than 8 times, a bound that some expert reaches in some of these blocks. `dispatched`: within each group of 4 consecutive blocks of 32 rows, blocks 2e and 2e + 1 are equal.
All inputs are finite; a program needn't handle non-finite values.
Results may differ from the reference program's by a relative error of at most 0.0058.
Values may be sent and summed in bfloat16 or wider, within the bound.
A program may use at most 64 MiB of HBM per device.

```python
import math
import jax
import jax.numpy as jnp
import numpy as np
from jax import lax

D = 1024
F = 512
NEXP = 128
TOPK = 8
MB = 4
TOK_DEV = 64
CAPS = 8
EXPERTS = 2
TOKENS = 2048
N_DP = 8
N_EXPERT = 4


def draw_dispatched(key, part):
    shape = (MB, N_DP, N_EXPERT // 2, N_EXPERT * CAPS, D)
    values = jax.random.truncated_normal(key, -4.0, 4.0, shape, jnp.float32)
    doubled = jnp.repeat(values, 2, axis=2)
    return doubled.reshape(MB, N_DP * N_EXPERT * N_EXPERT * CAPS, D).astype(jnp.bfloat16)


def levels(key, shape, shards, smallest, largest):
    gain, own = 1.0, jax.random.fold_in(key, 6)
    for dim, blocks in shards:
        steps = jnp.exp(jax.random.uniform(jax.random.fold_in(own, dim), (blocks,), jnp.float32, smallest / len(shards), largest / len(shards)))
        gain = gain * jnp.repeat(steps, shape[dim] // blocks).reshape([-1 if axis == dim else 1 for axis in range(len(shape))])
    return gain


def shared_out(rng, own, number, rows, number_of, top, limit, skew):
    sequence = jax.random.permutation(rng, number_of)
    heavy_load, ordinary = portions_of(number_of, rows * top, limit, skew, True), portions_of(number_of, rows * top, limit, skew, False)
    places = jnp.arange(number_of)

    def named(lengths, rotation):
        used = int((lengths > 0).sum())
        fixed = max(1, used // 4)
        passed = fixed + (places - fixed + rotation * (used - fixed)) % max(1, number_of - fixed)
        return jnp.zeros((number_of,), jnp.int32).at[sequence[jnp.where(places < fixed, places, passed)]].set(jnp.asarray(lengths, jnp.int32))

    lengths = jnp.where(number % 4 == 0, named(heavy_load, number // 4), named(ordinary, number - number // 4 - 1))
    mixed = jax.random.permutation(jax.random.fold_in(own, 3), number_of)
    source_of, taker = mixed[0:number_of // 2 * 2:2], mixed[1:number_of // 2 * 2:2]
    margin = jnp.minimum(lengths[source_of] - 1, limit - lengths[taker]) // 2
    margin = jnp.where((source_of == sequence[0]) | (taker == sequence[0]) | (lengths[taker] == 0), 0, jnp.maximum(margin, 0))
    passed = jax.random.randint(jax.random.fold_in(own, 4), (number_of // 2,), 0, 1 << 20) % (margin + 1)
    lengths = lengths.at[source_of].add(-passed).at[taker].add(passed)
    items = jnp.searchsorted(jnp.cumsum(lengths), jnp.arange(rows * top), side="right").astype(jnp.int32)
    table = items.reshape(top, rows).T
    table = table[jax.random.permutation(jax.random.fold_in(own, 1), rows)]
    rotation = jax.random.randint(jax.random.fold_in(own, 2), (rows, 1), 0, top)
    return jnp.take_along_axis(table, (jnp.arange(top)[None, :] + rotation) % top, axis=1)


def portions_of(count, total, reach, lean, full):
    loads = [(1 << 20) // math.isqrt(grade ** lean) + 1 for grade in range(1, count + 1)]
    largest = reach if full else min(reach, max(-(-total // count), total * loads[0] // sum(loads)))
    least = 1 if total - largest >= count - 1 else 0
    given, spare = [largest] + [least] * (count - 1), total - largest - least * (count - 1)
    while spare > 0:
        free = [i for i in range(1, count) if given[i] < largest] or [i for i in range(1, count) if given[i] < reach]
        pool, left = sum([loads[i] for i in free]), spare
        for i in free:
            addition = min(reach - given[i], max(1, left * loads[i] // pool), spare)
            given[i] = given[i] + addition
            spare = spare - addition
    return np.array(given)


def scatter_about(own_key, extent, deviation, bound, cuts=(), kind=jnp.bfloat16):
    result = jax.random.normal(own_key, extent, jnp.float32) * deviation
    if len(cuts) > 0:
        result = levels(own_key, extent, cuts, -0.22, 0.18) * result
    return jnp.clip(result, min=-bound, max=bound).astype(kind)


def setup_inputs(seed: int = 0) -> dict:
    splits = jax.random.split(jax.random.key(seed), 8)
    grad_out = scatter_about(splits[0], (MB, TOKENS, D), 3.0, 12.0, ((1, 32),))
    routes_keys = jax.random.split(jax.random.fold_in(splits[1], 1), MB * TOKENS // TOK_DEV)
    routes_turns = jax.random.permutation(jax.random.fold_in(splits[1], 3), MB * TOKENS // TOK_DEV)
    routes = jax.vmap(lambda own, number: shared_out(jax.random.fold_in(splits[1], 2), own, number, TOK_DEV, NEXP, TOPK, CAPS, 1))(routes_keys, routes_turns).reshape((MB, TOKENS, TOPK))
    route_probs = jnp.clip(0.049804688 + 0.3486328 * jax.random.uniform(splits[2], (MB, TOKENS, TOPK), jnp.float32) ** levels(splits[2], (MB, TOKENS, TOPK), ((1, 32),), -0.2, 0.2), 0.049804688, 0.3984375).astype(jnp.bfloat16)
    dispatched = draw_dispatched(jax.random.fold_in(splits[7], 71), 0)
    w_gate = scatter_about(splits[4], (D, EXPERTS * F), D ** -0.5, 0.1875, ((1, 4),))
    w_up = scatter_about(splits[5], (D, EXPERTS * F), D ** -0.5, 0.1875, ((1, 4),))
    w_down = scatter_about(splits[6], (EXPERTS * F, D), F ** -0.5, 0.25, ((0, 4),))
    return {"grad_out": grad_out, "routes": routes, "route_probs": route_probs, "dispatched": dispatched, "w_gate": w_gate, "w_up": w_up, "w_down": w_down}


def expert_backward(rows_in, row_grads, gate_mat, up_mat, down_mat):
    gate_pre = jnp.dot(rows_in, gate_mat, preferred_element_type=jnp.float32)
    up_pre = jnp.dot(rows_in, up_mat, preferred_element_type=jnp.float32)
    sigmoid = jax.nn.sigmoid(gate_pre)
    activated = gate_pre * sigmoid
    hidden = (activated * up_pre).astype(jnp.bfloat16)
    d_down = jnp.dot(row_grads.T, hidden, preferred_element_type=jnp.float32)
    dhidden = jnp.dot(row_grads, down_mat.T, preferred_element_type=jnp.float32)
    d_gate = (dhidden * up_pre * sigmoid * (1.0 + gate_pre * (1.0 - sigmoid))).astype(jnp.bfloat16)
    d_up = (dhidden * activated).astype(jnp.bfloat16)
    grad_gate_e = jnp.dot(rows_in.T, d_gate, preferred_element_type=jnp.float32)
    grad_up_e = jnp.dot(rows_in.T, d_up, preferred_element_type=jnp.float32)
    slot_grad = jnp.dot(d_gate, gate_mat.T, preferred_element_type=jnp.float32) + jnp.dot(d_up, up_mat.T, preferred_element_type=jnp.float32)
    return slot_grad, grad_gate_e, grad_up_e, d_down


def reference(grad_out, routes, route_probs, dispatched, w_gate, w_up, w_down):
    groups = N_EXPERT
    window = N_EXPERT // 2
    row_count = N_EXPERT * CAPS
    gate_blocks = w_gate.reshape(D, window, F).transpose(1, 0, 2)
    up_blocks = w_up.reshape(D, window, F).transpose(1, 0, 2)
    down_blocks = w_down.reshape(window, F, D)
    inputs = dispatched.reshape(MB * N_DP, groups, row_count, D)[:, ::2]
    out_grads = grad_out.reshape(MB * N_DP, groups * TOK_DEV, D)
    route_ids = routes.reshape(MB * N_DP, groups, TOK_DEV * TOPK)
    weights_all = route_probs.reshape(MB * N_DP, groups, TOK_DEV, TOPK)

    def group_step(totals, pieces):
        group_x, group_dy, group_ids, group_probs = pieces
        hitting = (group_ids[:, :, None] == jnp.arange(window, dtype=jnp.int32)[None, None, :]).astype(jnp.int32)
        ranking = jnp.sum((jnp.cumsum(hitting, axis=1) - 1) * hitting, axis=2)
        source = jnp.arange(groups, dtype=jnp.int32)[:, None]
        where_to = jnp.where(group_ids < window, group_ids * row_count + source * CAPS + ranking, window * row_count).astype(jnp.int32)
        scaled = (group_probs[..., None].astype(jnp.float32) * group_dy.reshape(groups, TOK_DEV, 1, D).astype(jnp.float32)).astype(jnp.bfloat16)
        buffer = jnp.zeros((window * row_count + 1, D), jnp.bfloat16).at[where_to.reshape(-1)].set(scaled.reshape(-1, D))
        slot_grads = buffer[:-1].reshape(window, row_count, D)

        def one_expert(packed):
            return expert_backward(packed[0], packed[1], packed[2], packed[3], packed[4])

        slot_grad, grad_gate_e, grad_up_e, d_down = lax.map(one_expert, (group_x, slot_grads, gate_blocks, up_blocks, down_blocks))
        padded = jnp.concatenate([slot_grad.reshape(window * row_count, D), jnp.zeros((1, D), jnp.float32)], axis=0)
        per_route = padded[where_to.reshape(-1)].reshape(groups * TOK_DEV, TOPK, D)
        grad_tokens = jnp.sum(per_route, axis=1).astype(jnp.bfloat16)
        totals = (totals[0] + grad_gate_e, totals[1] + grad_up_e, totals[2] + d_down)
        return totals, grad_tokens

    start = (jnp.zeros((window, D, F), jnp.float32), jnp.zeros((window, D, F), jnp.float32), jnp.zeros((window, D, F), jnp.float32))
    totals, grad_tokens = lax.scan(group_step, start, (inputs, out_grads, route_ids, weights_all))
    factor = 1.0 / (MB * N_DP)
    grad_gate = (totals[0] * factor).transpose(1, 0, 2).reshape(D, window * F)
    grad_up = (totals[1] * factor).transpose(1, 0, 2).reshape(D, window * F)
    grad_down_t = (totals[2] * factor).transpose(1, 0, 2).reshape(D, window * F)
    grad_in = grad_tokens.reshape(MB, N_DP * groups * TOK_DEV, D)
    return grad_in, grad_gate, grad_up, grad_down_t
```

```python
import functools

import jax
import jax.numpy as jnp
from jax import lax
from jax.experimental import pallas as pl
from jax.experimental.pallas import tpu as pltpu
from jax.sharding import PartitionSpec as P

CAPS = 8
MESH = pl.DeviceIdType.MESH
BF16 = jnp.bfloat16
F32 = jnp.float32


def dot(left, right, lc, rc):
    return lax.dot_general(
        left, right, (((lc,), (rc,)), ((), ())), preferred_element_type=F32
    )


def kernel(
    micro,
    n_exp,
    n_dp,
    routes_ref,
    probs_ref,
    go_hbm,
    x_hbm,
    wg_hbm,
    wu_hbm,
    wd_hbm,
    gin_ref,
    gg_ref,
    gu_ref,
    gd_ref,
    go_v,
    x_v,
    wg_v,
    wu_v,
    wd_v,
    a_send,
    a_buf,
    r_send,
    r_buf,
    acc,
    p1_send,
    p1_buf,
    p2_send,
    p2_buf,
    load_sem,
    a_ssem,
    a_rsem,
    r_ssem,
    r_rsem,
    p1_ssem,
    p1_rsem,
    p2_ssem,
    p2_rsem,
):
    member = lax.axis_index("expert")
    replica = lax.axis_index("dp")
    core = lax.rem(replica, 2)
    chip = lax.div(replica, 2)
    chips = n_dp // 2
    partner = {"dp": chip * 2 + 1 - core}
    window = n_exp // 2
    tokens = go_v.shape[0]
    width = go_v.shape[1]
    tok_dev = tokens // micro
    part = micro * CAPS
    rows = n_exp * part
    row_block = width // n_dp

    def member_at(k):
        return lax.rem(member + k, n_exp)

    def chip_at(k):
        return {"dp": lax.rem(chip + k, chips) * 2 + core}

    loads = [
        pltpu.make_async_copy(src, dst, load_sem.at[i])
        for i, (src, dst) in enumerate(
            ((go_hbm, go_v), (x_hbm, x_v), (wg_hbm, wg_v), (wu_hbm, wu_v), (wd_hbm, wd_v))
        )
    ]
    for load in loads:
        load.start()

    barrier = pltpu.get_barrier_semaphore()
    for k in range(1, n_exp):
        pl.semaphore_signal(
            barrier, inc=1, device_id={"expert": member_at(k)}, device_id_type=MESH
        )
    pl.semaphore_signal(barrier, inc=1, device_id=partner, device_id_type=MESH)
    for k in range(1, chips):
        pl.semaphore_signal(barrier, inc=1, device_id=chip_at(k), device_id_type=MESH)

    column = lax.broadcasted_iota(jnp.int32, (tokens, rows), 1)
    token = lax.broadcasted_iota(jnp.int32, (tokens, rows), 0)
    expert_of = lax.div(column, 2 * part)
    ids = routes_ref[...]
    probs = probs_ref[...].astype(F32)
    hits = jnp.zeros((tokens, rows), F32)
    weights = jnp.zeros((tokens, rows), F32)
    for e in range(window):
        named = ids == e
        hit = jnp.sum(jnp.where(named, 1.0, 0.0), axis=1, keepdims=True)
        weight = jnp.sum(jnp.where(named, probs, 0.0), axis=1, keepdims=True)
        hits = jnp.where(expert_of == e, hit, hits)
        weights = jnp.where(expert_of == e, weight, weights)
    ti = lax.broadcasted_iota(jnp.int32, (tokens, tokens), 0)
    tj = lax.broadcasted_iota(jnp.int32, (tokens, tokens), 1)
    earlier = jnp.where((ti > tj) & (lax.div(ti, tok_dev) == lax.div(tj, tok_dev)), 1.0, 0.0)
    ranking = dot(earlier.astype(BF16), hits.astype(BF16), 1, 0)
    chosen = (
        (hits > 0.5)
        & (ranking == lax.rem(column, CAPS).astype(F32))
        & (lax.div(token, tok_dev) == lax.rem(lax.div(column, CAPS), micro))
    )
    mixing = jnp.where(chosen, 1.0, 0.0).astype(BF16)
    picking = jnp.where(chosen, weights, 0.0).astype(BF16)

    loads[0].wait()
    sending = dot(picking, go_v[...], 0, 0).astype(BF16)
    for h in range(n_exp):
        a_send[h] = sending[h * part : (h + 1) * part]
    pl.semaphore_wait(barrier, n_exp - 1 + chips)
    a_copies = []
    for k in range(1, n_exp):
        copy = pltpu.make_async_remote_copy(
            src_ref=a_send.at[member_at(k)],
            dst_ref=a_buf.at[member],
            send_sem=a_ssem.at[k - 1],
            recv_sem=a_rsem.at[k - 1],
            device_id={"expert": member_at(k)},
            device_id_type=MESH,
        )
        copy.start()
        a_copies.append(copy)
    a_buf[member] = a_send[member]

    loads[1].wait()
    ri = lax.broadcasted_iota(jnp.int32, (rows, rows), 0)
    rj = lax.broadcasted_iota(jnp.int32, (rows, rows), 1)
    wanted = (
        lax.rem(lax.div(ri, CAPS), micro) * (n_exp * CAPS)
        + lax.div(ri, part) * CAPS
        + lax.rem(ri, CAPS)
    )
    inputs = dot(jnp.where(rj == wanted, 1.0, 0.0).astype(BF16), x_v[...], 1, 0).astype(BF16)
    loads[2].wait()
    gate = dot(inputs, wg_v[...], 1, 0)
    loads[3].wait()
    up = dot(inputs, wu_v[...], 1, 0)
    sigmoid = jax.nn.sigmoid(gate)
    activated = gate * sigmoid
    hidden = (activated * up).astype(BF16)
    slope = up * sigmoid * (1.0 + gate * (1.0 - sigmoid))
    loads[4].wait()

    def p1_copy(o):
        return pltpu.make_async_remote_copy(
            src_ref=p1_send.at[o, 1 - core],
            dst_ref=p1_buf.at[o],
            send_sem=p1_ssem.at[o],
            recv_sem=p1_rsem.at[o],
            device_id=partner,
            device_id_type=MESH,
        )

    def store_terms(o, value):
        for d in range(n_dp):
            block = value[d * row_block : (d + 1) * row_block]
            acc[o, d % 2, d // 2] = block
            p1_send[o, d % 2, d // 2] = block.astype(BF16)

    for copy in a_copies:
        copy.wait_recv()
    scaled = a_buf[...].reshape(rows, width)
    store_terms(0, dot(scaled, hidden, 0, 0))
    p1_copies = [p1_copy(0)]
    p1_copies[0].start()

    dhidden = dot(scaled, wd_v[...], 1, 1)
    d_gate = (dhidden * slope).astype(BF16)
    d_up = (dhidden * activated).astype(BF16)
    returning = (dot(d_gate, wg_v[...], 1, 1) + dot(d_up, wu_v[...], 1, 1)).astype(BF16)
    for h in range(n_exp):
        r_send[h] = returning[h * part : (h + 1) * part]
    r_copies = []
    for k in range(1, n_exp):
        copy = pltpu.make_async_remote_copy(
            src_ref=r_send.at[member_at(k)],
            dst_ref=r_buf.at[member],
            send_sem=r_ssem.at[k - 1],
            recv_sem=r_rsem.at[k - 1],
            device_id={"expert": member_at(k)},
            device_id_type=MESH,
        )
        copy.start()
        r_copies.append(copy)
    r_buf[member] = r_send[member]

    for o, grads in ((1, d_gate), (2, d_up)):
        store_terms(o, dot(inputs, grads, 0, 0))
        p1_copies.append(p1_copy(o))
        p1_copies[o].start()

    p2_copies = []
    for o in range(3):
        p1_copies[o].wait_recv()
        for q in range(chips):
            p2_send[o, q] = (acc[o, core, q] + p1_buf[o, q].astype(F32)).astype(BF16)
        for k in range(1, chips):
            copy = pltpu.make_async_remote_copy(
                src_ref=p2_send.at[o, lax.rem(chip + k, chips)],
                dst_ref=p2_buf.at[o, k - 1],
                send_sem=p2_ssem.at[o, k - 1],
                recv_sem=p2_rsem.at[o, k - 1],
                device_id=chip_at(k),
                device_id_type=MESH,
            )
            copy.start()
            p2_copies.append(copy)

    for copy in r_copies:
        copy.wait_recv()
    gin_ref[...] = dot(mixing, r_buf[...].reshape(rows, width), 1, 0).astype(BF16)

    factor = 1.0 / (micro * n_dp)
    for o, out in enumerate((gd_ref, gg_ref, gu_ref)):
        total = acc[o, core, chip] + p1_buf[o, chip].astype(F32)
        for k in range(1, chips):
            p2_copies[o * (chips - 1) + k - 1].wait_recv()
            total = total + p2_buf[o, k - 1].astype(F32)
        out[...] = total * factor
    for copy in a_copies + r_copies + p1_copies + p2_copies:
        copy.wait_send()


def per_device(n_exp, n_dp, grad_out, routes, route_probs, dispatched, w_gate, w_up, w_down):
    micro, tok_dev, width = grad_out.shape
    cols = w_gate.shape[1]
    tokens = micro * tok_dev
    part = micro * CAPS
    rows = n_exp * part
    chips = n_dp // 2
    row_block = width // n_dp
    vmem = pl.BlockSpec(memory_space=pltpu.VMEM)
    hbm = pl.BlockSpec(memory_space=pl.ANY)
    grad = jax.ShapeDtypeStruct((row_block, cols), F32)
    dma = pltpu.SemaphoreType.DMA
    others = max(chips - 1, 1)
    out = pl.pallas_call(
        functools.partial(kernel, micro, n_exp, n_dp),
        out_shape=(jax.ShapeDtypeStruct((tokens, width), BF16), grad, grad, grad),
        in_specs=[vmem, vmem, hbm, hbm, hbm, hbm, hbm],
        out_specs=(vmem, vmem, vmem, vmem),
        scratch_shapes=[
            pltpu.VMEM((tokens, width), BF16),
            pltpu.VMEM((rows, width), BF16),
            pltpu.VMEM((width, cols), BF16),
            pltpu.VMEM((width, cols), BF16),
            pltpu.VMEM((cols, width), BF16),
            pltpu.VMEM((n_exp, part, width), BF16),
            pltpu.VMEM((n_exp, part, width), BF16),
            pltpu.VMEM((n_exp, part, width), BF16),
            pltpu.VMEM((n_exp, part, width), BF16),
            pltpu.VMEM((3, 2, chips, row_block, cols), F32),
            pltpu.VMEM((3, 2, chips, row_block, cols), BF16),
            pltpu.VMEM((3, chips, row_block, cols), BF16),
            pltpu.VMEM((3, chips, row_block, cols), BF16),
            pltpu.VMEM((3, others, row_block, cols), BF16),
            dma((5,)),
            dma((n_exp - 1,)),
            dma((n_exp - 1,)),
            dma((n_exp - 1,)),
            dma((n_exp - 1,)),
            dma((3,)),
            dma((3,)),
            dma((3, others)),
            dma((3, others)),
        ],
        compiler_params=pltpu.CompilerParams(collective_id=0, has_side_effects=True),
    )(
        routes.reshape(tokens, -1),
        route_probs.reshape(tokens, -1),
        grad_out.reshape(tokens, width),
        dispatched.reshape(rows, width),
        w_gate,
        w_up,
        w_down,
    )
    return (out[0].reshape(micro, tok_dev, width),) + tuple(out[1:])


def solution(mesh):
    return jax.shard_map(
        functools.partial(per_device, mesh.shape["expert"], mesh.shape["dp"]),
        mesh=mesh,
        in_specs=(
            P(None, ("dp", "expert"), None),
            P(None, ("dp", "expert"), None),
            P(None, ("dp", "expert"), None),
            P(None, ("dp", "expert"), None),
            P(None, "expert"),
            P(None, "expert"),
            P("expert", None),
        ),
        out_specs=(
            P(None, ("dp", "expert"), None),
            P("dp", "expert"),
            P("dp", "expert"),
            P("dp", "expert"),
        ),
        check_vma=False,
    )
```

```python
import functools

import jax
import jax.numpy as jnp
from jax import lax
from jax.experimental import pallas as pl
from jax.experimental.pallas import tpu as pltpu
from jax.sharding import PartitionSpec as P

CAPS = 8
MESH = pl.DeviceIdType.MESH
BF16 = jnp.bfloat16
F32 = jnp.float32


def dot(left, right, lc, rc):
    return lax.dot_general(
        left, right, (((lc,), (rc,)), ((), ())), preferred_element_type=F32
    )


def flipped(index, bits):
    step = 1
    while step <= bits:
        if bits & step:
            index = index + step - 2 * step * lax.rem(lax.div(index, step), 2)
        step *= 2
    return index


def kernel(
    micro,
    n_exp,
    n_dp,
    routes_ref,
    probs_ref,
    go_hbm,
    x_hbm,
    wg_hbm,
    wu_hbm,
    wd_hbm,
    gin_ref,
    gg_ref,
    gu_ref,
    gd_ref,
    go_v,
    x_v,
    wg_v,
    wu_v,
    wd_v,
    a_send,
    a_buf,
    r_send,
    r_buf,
    acc,
    p1_send,
    p1_buf,
    p2_send,
    p2_buf,
    load_sem,
    a_ssem,
    a_rsem,
    r_ssem,
    r_rsem,
    p1_ssem,
    p1_rsem,
    p2_ssem,
    p2_rsem,
):
    member = lax.axis_index("expert")
    replica = lax.axis_index("dp")
    core = lax.rem(replica, 2)
    chip = lax.div(replica, 2)
    chips = n_dp // 2
    partner = {"dp": chip * 2 + 1 - core}
    window = n_exp // 2
    tokens = go_v.shape[0]
    width = go_v.shape[1]
    tok_dev = tokens // micro
    part = micro * CAPS
    rows = n_exp * part
    row_block = width // n_dp

    def member_at(k):
        return flipped(member, k)

    def chip_at(k):
        return {"dp": flipped(chip, k) * 2 + core}

    loads = [
        pltpu.make_async_copy(src, dst, load_sem.at[i])
        for i, (src, dst) in enumerate(
            ((go_hbm, go_v), (x_hbm, x_v), (wg_hbm, wg_v), (wu_hbm, wu_v), (wd_hbm, wd_v))
        )
    ]
    for load in loads:
        load.start()

    barrier = pltpu.get_barrier_semaphore()
    for k in range(1, n_exp):
        pl.semaphore_signal(
            barrier, inc=1, device_id={"expert": member_at(k)}, device_id_type=MESH
        )
    pl.semaphore_signal(barrier, inc=1, device_id=partner, device_id_type=MESH)
    for k in range(1, chips):
        pl.semaphore_signal(barrier, inc=1, device_id=chip_at(k), device_id_type=MESH)

    ids = jnp.concatenate([routes_ref[m] for m in range(micro)], axis=1)
    probs = jnp.concatenate([probs_ref[m].astype(F32) for m in range(micro)], axis=1)
    pad = max(window, 8)
    expert_row = lax.broadcasted_iota(jnp.int32, (pad, tokens), 0)
    hits, weights = [], []
    table = jnp.zeros((pad, tokens), F32)
    for e in range(window):
        named = ids == e
        hits.append(jnp.sum(jnp.where(named, 1.0, 0.0), axis=0, keepdims=True))
        weights.append(jnp.sum(jnp.where(named, probs, 0.0), axis=0, keepdims=True))
        table = jnp.where(expert_row == e, hits[e], table)
    ti = lax.broadcasted_iota(jnp.int32, (tokens, tokens), 0)
    tj = lax.broadcasted_iota(jnp.int32, (tokens, tokens), 1)
    earlier = jnp.where((ti < tj) & (lax.div(ti, tok_dev) == lax.div(tj, tok_dev)), 1.0, 0.0)
    ranking = dot(table.astype(BF16), earlier.astype(BF16), 1, 0)
    slot = lax.broadcasted_iota(jnp.int32, (CAPS, tokens), 0).astype(F32)
    batch = lax.div(lax.broadcasted_iota(jnp.int32, (CAPS, tokens), 1), tok_dev)
    ones, scales = [], []
    for h in range(n_exp):
        e = h // 2
        chosen = (hits[e] > 0.5) & (ranking[e : e + 1] == slot)
        for m in range(micro):
            here = chosen & (batch == m)
            ones.append(jnp.where(here, 1.0, 0.0))
            scales.append(jnp.where(here, weights[e], 0.0))
    mixing = jnp.concatenate(ones, axis=0).astype(BF16)
    picking = jnp.concatenate(scales, axis=0).astype(BF16)

    loads[0].wait()
    sending = dot(picking, go_v[...], 1, 0).astype(BF16)
    for h in range(n_exp):
        a_send[h] = sending[h * part : (h + 1) * part]
    pl.semaphore_wait(barrier, n_exp - 1 + chips)
    a_copies = []
    for k in range(n_exp - 1, 0, -1):
        copy = pltpu.make_async_remote_copy(
            src_ref=a_send.at[member_at(k)],
            dst_ref=a_buf.at[member],
            send_sem=a_ssem.at[k - 1],
            recv_sem=a_rsem.at[k - 1],
            device_id={"expert": member_at(k)},
            device_id_type=MESH,
        )
        copy.start()
        a_copies.append(copy)
    a_buf[member] = a_send[member]

    loads[1].wait()
    ri = lax.broadcasted_iota(jnp.int32, (rows, rows), 0)
    rj = lax.broadcasted_iota(jnp.int32, (rows, rows), 1)
    wanted = (
        lax.rem(lax.div(ri, CAPS), micro) * (n_exp * CAPS)
        + lax.div(ri, part) * CAPS
        + lax.rem(ri, CAPS)
    )
    inputs = dot(jnp.where(rj == wanted, 1.0, 0.0).astype(BF16), x_v[...], 1, 0).astype(BF16)
    loads[2].wait()
    gate = dot(inputs, wg_v[...], 1, 0)
    loads[3].wait()
    up = dot(inputs, wu_v[...], 1, 0)
    sigmoid = jax.nn.sigmoid(gate)
    activated = gate * sigmoid
    hidden = (activated * up).astype(BF16)
    slope = up * sigmoid * (1.0 + gate * (1.0 - sigmoid))
    loads[4].wait()

    def p1_copy(o):
        return pltpu.make_async_remote_copy(
            src_ref=p1_send.at[o, 1 - core],
            dst_ref=p1_buf.at[o],
            send_sem=p1_ssem.at[o],
            recv_sem=p1_rsem.at[o],
            device_id=partner,
            device_id_type=MESH,
        )

    def store_terms(o, value):
        for d in range(n_dp):
            block = value[d * row_block : (d + 1) * row_block]
            acc[o, d % 2, d // 2] = block
            p1_send[o, d % 2, d // 2] = block.astype(BF16)

    p1_copies, p2_copies = [], []

    def start_p1(o, value):
        store_terms(o, value)
        p1_copies.append(p1_copy(o))
        p1_copies[o].start()

    def start_p2(o):
        p1_copies[o].wait_recv()
        for k in range(chips - 1, 0, -1):
            q = flipped(chip, k)
            p2_send[o, q] = (acc[o, core, q] + p1_buf[o, q].astype(F32)).astype(BF16)
            copy = pltpu.make_async_remote_copy(
                src_ref=p2_send.at[o, q],
                dst_ref=p2_buf.at[o, k - 1],
                send_sem=p2_ssem.at[o, k - 1],
                recv_sem=p2_rsem.at[o, k - 1],
                device_id=chip_at(k),
                device_id_type=MESH,
            )
            copy.start()
            p2_copies.append(copy)

    for copy in a_copies:
        copy.wait_recv()
    scaled = a_buf[...].reshape(rows, width)
    start_p1(0, dot(scaled, hidden, 0, 0))
    dhidden = dot(scaled, wd_v[...], 1, 1)
    d_gate = (dhidden * slope).astype(BF16)
    d_up = (dhidden * activated).astype(BF16)
    start_p1(1, dot(inputs, d_gate, 0, 0))
    start_p2(0)
    returning = (dot(d_gate, wg_v[...], 1, 1) + dot(d_up, wu_v[...], 1, 1)).astype(BF16)
    for h in range(n_exp):
        r_send[h] = returning[h * part : (h + 1) * part]
    r_copies = []
    for k in range(n_exp - 1, 0, -1):
        copy = pltpu.make_async_remote_copy(
            src_ref=r_send.at[member_at(k)],
            dst_ref=r_buf.at[member],
            send_sem=r_ssem.at[k - 1],
            recv_sem=r_rsem.at[k - 1],
            device_id={"expert": member_at(k)},
            device_id_type=MESH,
        )
        copy.start()
        r_copies.append(copy)
    start_p2(1)
    start_p1(2, dot(inputs, d_up, 0, 0))
    r_buf[member] = r_send[member]
    start_p2(2)

    for copy in r_copies:
        copy.wait_recv()
    gin_ref[...] = dot(mixing, r_buf[...].reshape(rows, width), 0, 0).astype(BF16)

    factor = 1.0 / (micro * n_dp)
    for o, out in enumerate((gd_ref, gg_ref, gu_ref)):
        total = acc[o, core, chip] + p1_buf[o, chip].astype(F32)
        for k in range(chips - 1, 0, -1):
            p2_copies[o * (chips - 1) + chips - 1 - k].wait_recv()
            total = total + p2_buf[o, k - 1].astype(F32)
        out[...] = total * factor
    for copy in a_copies + r_copies + p1_copies + p2_copies:
        copy.wait_send()


def per_device(n_exp, n_dp, grad_out, routes, route_probs, dispatched, w_gate, w_up, w_down):
    micro, tok_dev, width = grad_out.shape
    cols = w_gate.shape[1]
    tokens = micro * tok_dev
    part = micro * CAPS
    rows = n_exp * part
    chips = n_dp // 2
    row_block = width // n_dp
    vmem = pl.BlockSpec(memory_space=pltpu.VMEM)
    hbm = pl.BlockSpec(memory_space=pl.ANY)
    grad = pltpu.VMEM((row_block, cols), F32)
    dma = pltpu.SemaphoreType.DMA
    others = max(chips - 1, 1)
    out = pl.pallas_call(
        functools.partial(kernel, micro, n_exp, n_dp),
        out_shape=(pltpu.VMEM((tokens, width), BF16), grad, grad, grad),
        in_specs=[vmem, vmem, hbm, hbm, hbm, hbm, hbm],
        out_specs=(vmem, vmem, vmem, vmem),
        scratch_shapes=[
            pltpu.VMEM((tokens, width), BF16),
            pltpu.VMEM((rows, width), BF16),
            pltpu.VMEM((width, cols), BF16),
            pltpu.VMEM((width, cols), BF16),
            pltpu.VMEM((cols, width), BF16),
            pltpu.VMEM((n_exp, part, width), BF16),
            pltpu.VMEM((n_exp, part, width), BF16),
            pltpu.VMEM((n_exp, part, width), BF16),
            pltpu.VMEM((n_exp, part, width), BF16),
            pltpu.VMEM((3, 2, chips, row_block, cols), F32),
            pltpu.VMEM((3, 2, chips, row_block, cols), BF16),
            pltpu.VMEM((3, chips, row_block, cols), BF16),
            pltpu.VMEM((3, chips, row_block, cols), BF16),
            pltpu.VMEM((3, others, row_block, cols), BF16),
            dma((5,)),
            dma((n_exp - 1,)),
            dma((n_exp - 1,)),
            dma((n_exp - 1,)),
            dma((n_exp - 1,)),
            dma((3,)),
            dma((3,)),
            dma((3, others)),
            dma((3, others)),
        ],
        compiler_params=pltpu.CompilerParams(collective_id=0, has_side_effects=True),
    )(
        routes.transpose(0, 2, 1),
        route_probs.transpose(0, 2, 1),
        grad_out.reshape(tokens, width),
        dispatched.reshape(rows, width),
        w_gate,
        w_up,
        w_down,
    )
    return (out[0].reshape(micro, tok_dev, width),) + tuple(out[1:])


def solution(mesh):
    return jax.shard_map(
        functools.partial(per_device, mesh.shape["expert"], mesh.shape["dp"]),
        mesh=mesh,
        in_specs=(
            P(None, ("dp", "expert"), None),
            P(None, ("dp", "expert"), None),
            P(None, ("dp", "expert"), None),
            P(None, ("dp", "expert"), None),
            P(None, "expert"),
            P(None, "expert"),
            P("expert", None),
        ),
        out_specs=(
            P(None, ("dp", "expert"), None),
            P("dp", "expert"),
            P("dp", "expert"),
            P("dp", "expert"),
        ),
        check_vma=False,
    )
```

```python
import functools

import jax
import jax.numpy as jnp
from jax import lax
from jax.experimental import pallas as pl
from jax.experimental.pallas import tpu as pltpu
from jax.sharding import PartitionSpec as P

CAPS = 8
MESH = pl.DeviceIdType.MESH
BF16 = jnp.bfloat16
F32 = jnp.float32


def dot(left, right, lc, rc):
    return lax.dot_general(
        left, right, (((lc,), (rc,)), ((), ())), preferred_element_type=F32
    )


def flipped(index, bits):
    step = 1
    while step <= bits:
        if bits & step:
            index = index + step - 2 * step * lax.rem(lax.div(index, step), 2)
        step *= 2
    return index


def kernel(
    micro,
    n_exp,
    n_dp,
    routes_ref,
    probs_ref,
    go_hbm,
    x_hbm,
    wg_hbm,
    wu_hbm,
    wd_hbm,
    gin_ref,
    gg_ref,
    gu_ref,
    gd_ref,
    go_v,
    x_v,
    wg_v,
    wu_v,
    wd_v,
    a_send,
    a_buf,
    r_send,
    r_buf,
    acc,
    p1_send,
    p1_buf,
    p2_send,
    p2_buf,
    s_all,
    h_all,
    load_sem,
    a_ssem,
    a_rsem,
    r_ssem,
    r_rsem,
    p1_ssem,
    p1_rsem,
    p2_ssem,
    p2_rsem,
    s_ssem,
    s_rsem,
    h_ssem,
    h_rsem,
):
    member = lax.axis_index("expert")
    replica = lax.axis_index("dp")
    core = lax.rem(replica, 2)
    chip = lax.div(replica, 2)
    chips = n_dp // 2
    partner = {"dp": chip * 2 + 1 - core}
    window = n_exp // 2
    tokens = go_v.shape[0]
    width = go_v.shape[1]
    tok_dev = tokens // micro
    part = micro * CAPS
    rows = n_exp * part
    row_block = width // n_dp
    gather = row_block % 128 == 0
    inner = lax.rem(lax.div(lax.rem(member, 4) + 1, 2), 2) == 1

    def member_at(k):
        return flipped(member, k)

    def chip_at(k):
        return {"dp": flipped(chip, k) * 2 + core}

    loads = [
        pltpu.make_async_copy(src, dst, load_sem.at[i])
        for i, (src, dst) in enumerate(
            ((go_hbm, go_v), (x_hbm, x_v), (wg_hbm, wg_v), (wu_hbm, wu_v), (wd_hbm, wd_v))
        )
    ]
    for load in loads:
        load.start()

    barrier = pltpu.get_barrier_semaphore()
    for k in range(1, n_exp):
        pl.semaphore_signal(
            barrier, inc=1, device_id={"expert": member_at(k)}, device_id_type=MESH
        )
    for k in range(1, n_dp):
        pl.semaphore_signal(
            barrier, inc=1, device_id={"dp": flipped(replica, k)}, device_id_type=MESH
        )

    ids = jnp.concatenate([routes_ref[m] for m in range(micro)], axis=1)
    probs = jnp.concatenate([probs_ref[m].astype(F32) for m in range(micro)], axis=1)
    pad = max(window, 8)
    expert_row = lax.broadcasted_iota(jnp.int32, (pad, tokens), 0)
    hits, weights = [], []
    table = jnp.zeros((pad, tokens), F32)
    for e in range(window):
        named = ids == e
        hits.append(jnp.sum(jnp.where(named, 1.0, 0.0), axis=0, keepdims=True))
        weights.append(jnp.sum(jnp.where(named, probs, 0.0), axis=0, keepdims=True))
        table = jnp.where(expert_row == e, hits[e], table)
    ti = lax.broadcasted_iota(jnp.int32, (tokens, tokens), 0)
    tj = lax.broadcasted_iota(jnp.int32, (tokens, tokens), 1)
    earlier = jnp.where((ti < tj) & (lax.div(ti, tok_dev) == lax.div(tj, tok_dev)), 1.0, 0.0)
    ranking = dot(table.astype(BF16), earlier.astype(BF16), 1, 0)
    slot = lax.broadcasted_iota(jnp.int32, (CAPS, tokens), 0).astype(F32)
    batch = lax.div(lax.broadcasted_iota(jnp.int32, (CAPS, tokens), 1), tok_dev)
    ones, scales = [], []
    for h in range(n_exp):
        e = h // 2
        chosen = (hits[e] > 0.5) & (ranking[e : e + 1] == slot)
        for m in range(micro):
            here = chosen & (batch == m)
            ones.append(jnp.where(here, 1.0, 0.0))
            scales.append(jnp.where(here, weights[e], 0.0))
    mixing = jnp.concatenate(ones, axis=0).astype(BF16)
    picking = jnp.concatenate(scales, axis=0).astype(BF16)

    loads[0].wait()
    sending = dot(picking, go_v[...], 1, 0).astype(BF16)
    for h in range(n_exp):
        a_send[h] = sending[h * part : (h + 1) * part]
    pl.semaphore_wait(barrier, n_exp - 1 + n_dp - 1)
    def a_copy(k, src, slot, to):
        return pltpu.make_async_remote_copy(
            src_ref=src,
            dst_ref=a_buf.at[slot],
            send_sem=a_ssem.at[k - 1],
            recv_sem=a_rsem.at[k - 1],
            device_id={"expert": to},
            device_id_type=MESH,
        )

    a_copies = {}
    for k in range(n_exp - 1, 0, -1):
        a_copies[k] = a_copy(k, a_send.at[member_at(k)], member, member_at(k))
        if k == 2:
            pl.when(jnp.logical_not(inner))(a_copies[k].start)
        else:
            a_copies[k].start()
    a_buf[member] = a_send[member]

    loads[1].wait()
    ri = lax.broadcasted_iota(jnp.int32, (rows, rows), 0)
    rj = lax.broadcasted_iota(jnp.int32, (rows, rows), 1)
    wanted = (
        lax.rem(lax.div(ri, CAPS), micro) * (n_exp * CAPS)
        + lax.div(ri, part) * CAPS
        + lax.rem(ri, CAPS)
    )
    inputs = dot(jnp.where(rj == wanted, 1.0, 0.0).astype(BF16), x_v[...], 1, 0).astype(BF16)
    if n_exp > 2:
        across = member_at(3)
        a_copies[3].wait_recv()
        passed = a_copy(2, a_buf.at[across], across, member_at(1))
        pl.when(inner)(passed.start)
    loads[2].wait()
    gate = dot(inputs, wg_v[...], 1, 0)
    loads[3].wait()
    up = dot(inputs, wu_v[...], 1, 0)
    sigmoid = jax.nn.sigmoid(gate)
    activated = gate * sigmoid
    hidden = (activated * up).astype(BF16)
    h_copies, s_copies = [], []
    if gather:
        h_all[replica] = hidden
        for k in range(n_dp - 1, 0, -1):
            copy = pltpu.make_async_remote_copy(
                src_ref=h_all.at[replica],
                dst_ref=h_all.at[replica],
                send_sem=h_ssem.at[k - 1],
                recv_sem=h_rsem.at[k - 1],
                device_id={"dp": flipped(replica, k)},
                device_id_type=MESH,
            )
            copy.start()
            h_copies.append(copy)
    slope = up * sigmoid * (1.0 + gate * (1.0 - sigmoid))
    loads[4].wait()

    def p1_copy(o):
        return pltpu.make_async_remote_copy(
            src_ref=p1_send.at[o, 1 - core],
            dst_ref=p1_buf.at[o],
            send_sem=p1_ssem.at[o],
            recv_sem=p1_rsem.at[o],
            device_id=partner,
            device_id_type=MESH,
        )

    def store_terms(o, value):
        for d in range(n_dp):
            block = value[d * row_block : (d + 1) * row_block]
            acc[o, d % 2, d // 2] = block
            p1_send[o, d % 2, d // 2] = block.astype(BF16)

    p1_copies, p2_copies = {}, {}

    def start_p1(o, value):
        store_terms(o, value)
        p1_copies[o] = p1_copy(o)
        p1_copies[o].start()

    def start_p2(o):
        p1_copies[o].wait_recv()
        for k in range(chips - 1, 0, -1):
            q = flipped(chip, k)
            p2_send[o, q] = (acc[o, core, q] + p1_buf[o, q].astype(F32)).astype(BF16)
            copy = pltpu.make_async_remote_copy(
                src_ref=p2_send.at[o, q],
                dst_ref=p2_buf.at[o, k - 1],
                send_sem=p2_ssem.at[o, k - 1],
                recv_sem=p2_rsem.at[o, k - 1],
                device_id=chip_at(k),
                device_id_type=MESH,
            )
            copy.start()
            p2_copies[o, k] = copy

    for k in range(1, n_exp):
        if k != 3:
            a_copies[k].wait_recv()
    scaled = a_buf[...].reshape(rows, width)
    if gather:
        for k in range(n_dp - 1, 0, -1):
            peer = flipped(replica, k)
            columns = pl.ds(pl.multiple_of(peer * row_block, row_block), row_block)
            copy = pltpu.make_async_remote_copy(
                src_ref=a_buf.at[:, :, columns],
                dst_ref=s_all.at[replica],
                send_sem=s_ssem.at[k - 1],
                recv_sem=s_rsem.at[k - 1],
                device_id={"dp": peer},
                device_id_type=MESH,
            )
            copy.start()
            s_copies.append(copy)
    else:
        start_p1(0, dot(scaled, hidden, 0, 0))
    dhidden = dot(scaled, wd_v[...], 1, 1)
    d_gate = (dhidden * slope).astype(BF16)
    d_up = (dhidden * activated).astype(BF16)
    returning = (dot(d_gate, wg_v[...], 1, 1) + dot(d_up, wu_v[...], 1, 1)).astype(BF16)
    for h in range(n_exp):
        r_send[h] = returning[h * part : (h + 1) * part]
    r_copies = []
    for k in range(n_exp - 1, 0, -1):
        copy = pltpu.make_async_remote_copy(
            src_ref=r_send.at[member_at(k)],
            dst_ref=r_buf.at[member],
            send_sem=r_ssem.at[k - 1],
            recv_sem=r_rsem.at[k - 1],
            device_id={"expert": member_at(k)},
            device_id_type=MESH,
        )
        copy.start()
        r_copies.append(copy)
    start_p1(1, dot(inputs, d_gate, 0, 0))
    start_p1(2, dot(inputs, d_up, 0, 0))
    if not gather:
        start_p2(0)
    r_buf[member] = r_send[member]
    start_p2(1)
    start_p2(2)

    if gather:
        own = pl.ds(pl.multiple_of(replica * row_block, row_block), row_block)
        s_all[replica] = a_buf[:, :, own]
        for copy in h_copies + s_copies:
            copy.wait_recv()
        slots = n_dp * rows
        down = dot(
            s_all[...].reshape(slots, row_block), h_all[...].reshape(slots, wg_v.shape[1]), 0, 0
        )
        gd_ref[...] = down * (1.0 / (micro * n_dp))
    for copy in r_copies:
        copy.wait_recv()
    gin_ref[...] = dot(mixing, r_buf[...].reshape(rows, width), 0, 0).astype(BF16)

    factor = 1.0 / (micro * n_dp)
    for o, out in enumerate((gd_ref, gg_ref, gu_ref)):
        if o not in p1_copies:
            continue
        total = acc[o, core, chip] + p1_buf[o, chip].astype(F32)
        for k in range(chips - 1, 0, -1):
            p2_copies[o, k].wait_recv()
            total = total + p2_buf[o, k - 1].astype(F32)
        out[...] = total * factor
    started = [*a_copies.values(), *p1_copies.values(), *p2_copies.values()]
    for copy in started + r_copies + h_copies + s_copies:
        copy.wait_send()


def settle(*refs):
    count = len(refs) // 2
    sem = refs[-1]
    copies = [
        pltpu.make_async_copy(refs[i], refs[count + i], sem.at[i]) for i in range(count)
    ]
    for copy in copies:
        copy.start()
    for copy in copies:
        copy.wait()


def settled(arrays):
    anywhere = pl.BlockSpec(memory_space=pl.ANY)
    return pl.pallas_call(
        settle,
        out_shape=tuple(jax.ShapeDtypeStruct(a.shape, a.dtype) for a in arrays),
        in_specs=[pl.BlockSpec(memory_space=pltpu.VMEM)] * len(arrays),
        out_specs=(anywhere,) * len(arrays),
        scratch_shapes=[pltpu.SemaphoreType.DMA((len(arrays),))],
    )(*[pltpu.with_memory_space_constraint(a, pltpu.VMEM) for a in arrays])


def per_device(n_exp, n_dp, grad_out, routes, route_probs, dispatched, w_gate, w_up, w_down):
    micro, tok_dev, width = grad_out.shape
    cols = w_gate.shape[1]
    tokens = micro * tok_dev
    part = micro * CAPS
    rows = n_exp * part
    chips = n_dp // 2
    row_block = width // n_dp
    vmem = pl.BlockSpec(memory_space=pltpu.VMEM)
    hbm = pl.BlockSpec(memory_space=pl.ANY)
    grad = pltpu.VMEM((row_block, cols), F32)
    dma = pltpu.SemaphoreType.DMA
    others = max(chips - 1, 1)
    gather = row_block % 128 == 0
    out = pl.pallas_call(
        functools.partial(kernel, micro, n_exp, n_dp),
        out_shape=(pltpu.VMEM((tokens, width), BF16), grad, grad, grad),
        in_specs=[vmem, vmem, hbm, hbm, hbm, hbm, hbm],
        out_specs=(vmem, vmem, vmem, vmem),
        scratch_shapes=[
            pltpu.VMEM((tokens, width), BF16),
            pltpu.VMEM((rows, width), BF16),
            pltpu.VMEM((width, cols), BF16),
            pltpu.VMEM((width, cols), BF16),
            pltpu.VMEM((cols, width), BF16),
            pltpu.VMEM((n_exp, part, width), BF16),
            pltpu.VMEM((n_exp, part, width), BF16),
            pltpu.VMEM((n_exp, part, width), BF16),
            pltpu.VMEM((n_exp, part, width), BF16),
            pltpu.VMEM((3, 2, chips, row_block, cols), F32),
            pltpu.VMEM((3, 2, chips, row_block, cols), BF16),
            pltpu.VMEM((3, chips, row_block, cols), BF16),
            pltpu.VMEM((3, chips, row_block, cols), BF16),
            pltpu.VMEM((3, others, row_block, cols), BF16),
            pltpu.VMEM((n_dp, n_exp, part, row_block) if gather else (8, 128), BF16),
            pltpu.VMEM((n_dp, rows, cols) if gather else (8, 128), BF16),
            dma((5,)),
            dma((n_exp - 1,)),
            dma((n_exp - 1,)),
            dma((n_exp - 1,)),
            dma((n_exp - 1,)),
            dma((3,)),
            dma((3,)),
            dma((3, others)),
            dma((3, others)),
            dma((n_dp - 1,)),
            dma((n_dp - 1,)),
            dma((n_dp - 1,)),
            dma((n_dp - 1,)),
        ],
        compiler_params=pltpu.CompilerParams(collective_id=0, has_side_effects=True),
    )(
        routes.transpose(0, 2, 1),
        route_probs.transpose(0, 2, 1),
        grad_out.reshape(tokens, width),
        dispatched.reshape(rows, width),
        w_gate,
        w_up,
        w_down,
    )
    out = settled(out)
    return (out[0].reshape(micro, tok_dev, width),) + tuple(out[1:])


def solution(mesh):
    return jax.shard_map(
        functools.partial(per_device, mesh.shape["expert"], mesh.shape["dp"]),
        mesh=mesh,
        in_specs=(
            P(None, ("dp", "expert"), None),
            P(None, ("dp", "expert"), None),
            P(None, ("dp", "expert"), None),
            P(None, ("dp", "expert"), None),
            P(None, "expert"),
            P(None, "expert"),
            P("expert", None),
        ),
        out_specs=(
            P(None, ("dp", "expert"), None),
            P("dp", "expert"),
            P("dp", "expert"),
            P("dp", "expert"),
        ),
        check_vma=False,
    )
```

```python
import functools

import jax
import jax.numpy as jnp
from jax import lax
from jax.experimental import pallas as pl
from jax.experimental.pallas import tpu as pltpu
from jax.sharding import PartitionSpec as P

CAPS = 8
MESH = pl.DeviceIdType.MESH
BF16 = jnp.bfloat16
F32 = jnp.float32


def dot(left, right, lc, rc):
    return lax.dot_general(
        left, right, (((lc,), (rc,)), ((), ())), preferred_element_type=F32
    )


def flipped(index, bits):
    step = 1
    while step <= bits:
        if bits & step:
            index = index + step - 2 * step * lax.rem(lax.div(index, step), 2)
        step *= 2
    return index


def kernel(
    micro,
    n_exp,
    n_dp,
    routes_ref,
    probs_ref,
    go_hbm,
    x_hbm,
    wg_hbm,
    wu_hbm,
    wd_hbm,
    gin_ref,
    gg_ref,
    gu_ref,
    gd_ref,
    go_v,
    x_v,
    wg_v,
    wu_v,
    wd_v,
    a_send,
    a_buf,
    r_send,
    r_buf,
    acc,
    p1_send,
    p1_buf,
    p2_send,
    p2_buf,
    s_all,
    h_all,
    load_sem,
    a_ssem,
    a_rsem,
    r_ssem,
    r_rsem,
    p1_ssem,
    p1_rsem,
    p2_ssem,
    p2_rsem,
    s_ssem,
    s_rsem,
    h_ssem,
    h_rsem,
):
    member = lax.axis_index("expert")
    replica = lax.axis_index("dp")
    core = lax.rem(replica, 2)
    chip = lax.div(replica, 2)
    chips = n_dp // 2
    partner = {"dp": chip * 2 + 1 - core}
    window = n_exp // 2
    tokens = go_v.shape[0]
    width = go_v.shape[1]
    tok_dev = tokens // micro
    part = micro * CAPS
    rows = n_exp * part
    row_block = width // n_dp
    gather = row_block % 128 == 0

    def member_at(k):
        return flipped(member, k)

    def chip_at(k):
        return {"dp": flipped(chip, k) * 2 + core}

    loads = [
        pltpu.make_async_copy(src, dst, load_sem.at[i])
        for i, (src, dst) in enumerate(
            ((go_hbm, go_v), (x_hbm, x_v), (wg_hbm, wg_v), (wu_hbm, wu_v), (wd_hbm, wd_v))
        )
    ]
    for load in loads:
        load.start()

    barrier = pltpu.get_barrier_semaphore()
    for k in range(1, n_exp):
        pl.semaphore_signal(
            barrier, inc=1, device_id={"expert": member_at(k)}, device_id_type=MESH
        )
    for k in range(1, n_dp):
        pl.semaphore_signal(
            barrier, inc=1, device_id={"dp": flipped(replica, k)}, device_id_type=MESH
        )

    ids = jnp.concatenate([routes_ref[m] for m in range(micro)], axis=1)
    probs = jnp.concatenate([probs_ref[m].astype(F32) for m in range(micro)], axis=1)
    pad = max(window, 8)
    expert_row = lax.broadcasted_iota(jnp.int32, (pad, tokens), 0)
    hits, weights = [], []
    table = jnp.zeros((pad, tokens), F32)
    for e in range(window):
        named = ids == e
        hits.append(jnp.sum(jnp.where(named, 1.0, 0.0), axis=0, keepdims=True))
        weights.append(jnp.sum(jnp.where(named, probs, 0.0), axis=0, keepdims=True))
        table = jnp.where(expert_row == e, hits[e], table)
    ti = lax.broadcasted_iota(jnp.int32, (tokens, tokens), 0)
    tj = lax.broadcasted_iota(jnp.int32, (tokens, tokens), 1)
    earlier = jnp.where((ti < tj) & (lax.div(ti, tok_dev) == lax.div(tj, tok_dev)), 1.0, 0.0)
    ranking = dot(table.astype(BF16), earlier.astype(BF16), 1, 0)
    slot = lax.broadcasted_iota(jnp.int32, (CAPS, tokens), 0).astype(F32)
    batch = lax.div(lax.broadcasted_iota(jnp.int32, (CAPS, tokens), 1), tok_dev)
    ones, scales = [], []
    for h in range(n_exp):
        e = h // 2
        chosen = (hits[e] > 0.5) & (ranking[e : e + 1] == slot)
        for m in range(micro):
            here = chosen & (batch == m)
            ones.append(jnp.where(here, 1.0, 0.0))
            scales.append(jnp.where(here, weights[e], 0.0))
    mixing = jnp.concatenate(ones, axis=0).astype(BF16)
    picking = jnp.concatenate(scales, axis=0).astype(BF16)

    loads[0].wait()
    sending = dot(picking, go_v[...], 1, 0).astype(BF16)
    for h in range(n_exp):
        a_send[h] = sending[h * part : (h + 1) * part]
    pl.semaphore_wait(barrier, n_exp - 1 + n_dp - 1)
    def a_copy(k, src, slot, to):
        return pltpu.make_async_remote_copy(
            src_ref=src,
            dst_ref=a_buf.at[slot],
            send_sem=a_ssem.at[k - 1],
            recv_sem=a_rsem.at[k - 1],
            device_id={"expert": to},
            device_id_type=MESH,
        )

    a_copies = {}
    for k in range(1, n_exp):
        a_copies[k] = a_copy(k, a_send.at[member_at(k)], member, member_at(k))
        a_copies[k].start()
    a_buf[member] = a_send[member]

    loads[1].wait()
    ri = lax.broadcasted_iota(jnp.int32, (rows, rows), 0)
    rj = lax.broadcasted_iota(jnp.int32, (rows, rows), 1)
    wanted = (
        lax.rem(lax.div(ri, CAPS), micro) * (n_exp * CAPS)
        + lax.div(ri, part) * CAPS
        + lax.rem(ri, CAPS)
    )
    inputs = dot(jnp.where(rj == wanted, 1.0, 0.0).astype(BF16), x_v[...], 1, 0).astype(BF16)
    loads[2].wait()
    gate = dot(inputs, wg_v[...], 1, 0)
    loads[3].wait()
    up = dot(inputs, wu_v[...], 1, 0)
    sigmoid = jax.nn.sigmoid(gate)
    activated = gate * sigmoid
    hidden = (activated * up).astype(BF16)
    h_copies, s_copies = [], []
    if gather:
        h_all[replica] = hidden
        for k in range(n_dp - 1, 0, -1):
            copy = pltpu.make_async_remote_copy(
                src_ref=h_all.at[replica],
                dst_ref=h_all.at[replica],
                send_sem=h_ssem.at[k - 1],
                recv_sem=h_rsem.at[k - 1],
                device_id={"dp": flipped(replica, k)},
                device_id_type=MESH,
            )
            copy.start()
            h_copies.append(copy)
    slope = up * sigmoid * (1.0 + gate * (1.0 - sigmoid))
    loads[4].wait()

    def p1_copy(o):
        return pltpu.make_async_remote_copy(
            src_ref=p1_send.at[o, 1 - core],
            dst_ref=p1_buf.at[o],
            send_sem=p1_ssem.at[o],
            recv_sem=p1_rsem.at[o],
            device_id=partner,
            device_id_type=MESH,
        )

    def store_terms(o, value):
        for d in range(n_dp):
            block = value[d * row_block : (d + 1) * row_block]
            acc[o, d % 2, d // 2] = block
            p1_send[o, d % 2, d // 2] = block.astype(BF16)

    p1_copies, p2_copies = {}, {}

    def start_p1(o, value):
        store_terms(o, value)
        p1_copies[o] = p1_copy(o)
        p1_copies[o].start()

    def start_p2(o):
        p1_copies[o].wait_recv()
        for k in range(chips - 1, 0, -1):
            q = flipped(chip, k)
            p2_send[o, q] = (acc[o, core, q] + p1_buf[o, q].astype(F32)).astype(BF16)
            copy = pltpu.make_async_remote_copy(
                src_ref=p2_send.at[o, q],
                dst_ref=p2_buf.at[o, k - 1],
                send_sem=p2_ssem.at[o, k - 1],
                recv_sem=p2_rsem.at[o, k - 1],
                device_id=chip_at(k),
                device_id_type=MESH,
            )
            copy.start()
            p2_copies[o, k] = copy

    for k in range(1, n_exp):
        a_copies[k].wait_recv()
    scaled = a_buf[...].reshape(rows, width)
    if gather:
        for k in range(n_dp - 1, 0, -1):
            peer = flipped(replica, k)
            columns = pl.ds(pl.multiple_of(peer * row_block, row_block), row_block)
            copy = pltpu.make_async_remote_copy(
                src_ref=a_buf.at[:, :, columns],
                dst_ref=s_all.at[replica],
                send_sem=s_ssem.at[k - 1],
                recv_sem=s_rsem.at[k - 1],
                device_id={"dp": peer},
                device_id_type=MESH,
            )
            copy.start()
            s_copies.append(copy)
    else:
        start_p1(0, dot(scaled, hidden, 0, 0))
    dhidden = dot(scaled, wd_v[...], 1, 1)
    d_gate = (dhidden * slope).astype(BF16)
    d_up = (dhidden * activated).astype(BF16)
    returning = (dot(d_gate, wg_v[...], 1, 1) + dot(d_up, wu_v[...], 1, 1)).astype(BF16)
    for h in range(n_exp):
        r_send[h] = returning[h * part : (h + 1) * part]
    r_copies = []
    for k in range(n_exp - 1, 0, -1):
        copy = pltpu.make_async_remote_copy(
            src_ref=r_send.at[member_at(k)],
            dst_ref=r_buf.at[member],
            send_sem=r_ssem.at[k - 1],
            recv_sem=r_rsem.at[k - 1],
            device_id={"expert": member_at(k)},
            device_id_type=MESH,
        )
        copy.start()
        r_copies.append(copy)
    start_p1(1, dot(inputs, d_gate, 0, 0))
    start_p1(2, dot(inputs, d_up, 0, 0))
    if not gather:
        start_p2(0)
    r_buf[member] = r_send[member]
    start_p2(1)
    start_p2(2)

    if gather:
        own = pl.ds(pl.multiple_of(replica * row_block, row_block), row_block)
        s_all[replica] = a_buf[:, :, own]
        for copy in h_copies + s_copies:
            copy.wait_recv()
        slots = n_dp * rows
        down = dot(
            s_all[...].reshape(slots, row_block), h_all[...].reshape(slots, wg_v.shape[1]), 0, 0
        )
        gd_ref[...] = down * (1.0 / (micro * n_dp))
    for copy in r_copies:
        copy.wait_recv()
    gin_ref[...] = dot(mixing, r_buf[...].reshape(rows, width), 0, 0).astype(BF16)

    factor = 1.0 / (micro * n_dp)
    for o, out in enumerate((gd_ref, gg_ref, gu_ref)):
        if o not in p1_copies:
            continue
        total = acc[o, core, chip] + p1_buf[o, chip].astype(F32)
        for k in range(chips - 1, 0, -1):
            p2_copies[o, k].wait_recv()
            total = total + p2_buf[o, k - 1].astype(F32)
        out[...] = total * factor
    started = [*a_copies.values(), *p1_copies.values(), *p2_copies.values()]
    for copy in started + r_copies + h_copies + s_copies:
        copy.wait_send()


def settle(*refs):
    count = len(refs) // 2
    sem = refs[-1]
    copies = [
        pltpu.make_async_copy(refs[i], refs[count + i], sem.at[i]) for i in range(count)
    ]
    for copy in copies:
        copy.start()
    for copy in copies:
        copy.wait()


def settled(arrays):
    anywhere = pl.BlockSpec(memory_space=pl.ANY)
    return pl.pallas_call(
        settle,
        out_shape=tuple(jax.ShapeDtypeStruct(a.shape, a.dtype) for a in arrays),
        in_specs=[pl.BlockSpec(memory_space=pltpu.VMEM)] * len(arrays),
        out_specs=(anywhere,) * len(arrays),
        scratch_shapes=[pltpu.SemaphoreType.DMA((len(arrays),))],
    )(*[pltpu.with_memory_space_constraint(a, pltpu.VMEM) for a in arrays])


def per_device(n_exp, n_dp, grad_out, routes, route_probs, dispatched, w_gate, w_up, w_down):
    micro, tok_dev, width = grad_out.shape
    cols = w_gate.shape[1]
    tokens = micro * tok_dev
    part = micro * CAPS
    rows = n_exp * part
    chips = n_dp // 2
    row_block = width // n_dp
    vmem = pl.BlockSpec(memory_space=pltpu.VMEM)
    hbm = pl.BlockSpec(memory_space=pl.ANY)
    grad = pltpu.VMEM((row_block, cols), F32)
    dma = pltpu.SemaphoreType.DMA
    others = max(chips - 1, 1)
    gather = row_block % 128 == 0
    out = pl.pallas_call(
        functools.partial(kernel, micro, n_exp, n_dp),
        out_shape=(pltpu.VMEM((tokens, width), BF16), grad, grad, grad),
        in_specs=[vmem, vmem, hbm, hbm, hbm, hbm, hbm],
        out_specs=(vmem, vmem, vmem, vmem),
        scratch_shapes=[
            pltpu.VMEM((tokens, width), BF16),
            pltpu.VMEM((rows, width), BF16),
            pltpu.VMEM((width, cols), BF16),
            pltpu.VMEM((width, cols), BF16),
            pltpu.VMEM((cols, width), BF16),
            pltpu.VMEM((n_exp, part, width), BF16),
            pltpu.VMEM((n_exp, part, width), BF16),
            pltpu.VMEM((n_exp, part, width), BF16),
            pltpu.VMEM((n_exp, part, width), BF16),
            pltpu.VMEM((3, 2, chips, row_block, cols), F32),
            pltpu.VMEM((3, 2, chips, row_block, cols), BF16),
            pltpu.VMEM((3, chips, row_block, cols), BF16),
            pltpu.VMEM((3, chips, row_block, cols), BF16),
            pltpu.VMEM((3, others, row_block, cols), BF16),
            pltpu.VMEM((n_dp, n_exp, part, row_block) if gather else (8, 128), BF16),
            pltpu.VMEM((n_dp, rows, cols) if gather else (8, 128), BF16),
            dma((5,)),
            dma((n_exp - 1,)),
            dma((n_exp - 1,)),
            dma((n_exp - 1,)),
            dma((n_exp - 1,)),
            dma((3,)),
            dma((3,)),
            dma((3, others)),
            dma((3, others)),
            dma((n_dp - 1,)),
            dma((n_dp - 1,)),
            dma((n_dp - 1,)),
            dma((n_dp - 1,)),
        ],
        compiler_params=pltpu.CompilerParams(collective_id=0, has_side_effects=True),
    )(
        routes.transpose(0, 2, 1),
        route_probs.transpose(0, 2, 1),
        grad_out.reshape(tokens, width),
        dispatched.reshape(rows, width),
        w_gate,
        w_up,
        w_down,
    )
    out = settled(out)
    return (out[0].reshape(micro, tok_dev, width),) + tuple(out[1:])


def solution(mesh):
    return jax.shard_map(
        functools.partial(per_device, mesh.shape["expert"], mesh.shape["dp"]),
        mesh=mesh,
        in_specs=(
            P(None, ("dp", "expert"), None),
            P(None, ("dp", "expert"), None),
            P(None, ("dp", "expert"), None),
            P(None, ("dp", "expert"), None),
            P(None, "expert"),
            P(None, "expert"),
            P("expert", None),
        ),
        out_specs=(
            P(None, ("dp", "expert"), None),
            P("dp", "expert"),
            P("dp", "expert"),
            P("dp", "expert"),
        ),
        check_vma=False,
    )
```
